32 devices in a mesh: ctx: 8 (over z, y), dp: 4 (over x, core).
Axes of the slice: x: 2, y: 2, z: 4, core: 2. Of those that a mesh axis runs over, the one named last changes fastest.
Arguments:
- grad_out: bfloat16 [4, 3072, 4096], P('dp', 'ctx'), may hold values from -6 to 6
- hidden: bfloat16 [4, 3072, 1792], P('dp', 'ctx'), may hold values from -6 to 6
- down_weight: bfloat16 [1792, 4096], replicated, may hold values from -0.09375 to 0.09375
Outputs:
- grad_hidden: bfloat16 [4, 3072, 1792], P('dp', 'ctx')
- weight_grad: float32 [1792, 4096], P('ctx', 'dp')
- hidden_amax: float32 [4, 1792], P('dp', 'ctx')
- grad_amax: float32 [4, 4096], P('dp', 'ctx')
The draws below stay inside these ranges and needn't reach their ends.
All inputs are finite; a program needn't handle non-finite values.
Results may differ from the reference program's by a relative error of at most 0.006.
Values may be sent and summed in bfloat16 or wider, within the bound.
A program may use at most 192 MiB of HBM per device.

```python
import jax
import jax.numpy as jnp
from jax import lax

D = 4096
FFS = 1792
SEQ = 3072
REPLICAS = 4


def level_of(own_key, dims, pieces, low, top_value):
    level, own = 1.0, jax.random.fold_in(own_key, 6)
    for dim, shards_of in pieces:
        heights = jnp.exp(jax.random.uniform(jax.random.fold_in(own, dim), (shards_of,), jnp.float32, low / len(pieces), top_value / len(pieces)))
        level = level * jnp.repeat(heights, dims[dim] // shards_of).reshape([-1 if axis == dim else 1 for axis in range(len(dims))])
    return level


def noise(stream_key, extent, spread, reach, split=(), dtype=jnp.bfloat16):
    array = spread * jax.random.normal(stream_key, extent, jnp.float32)
    if split:
        array = array * level_of(stream_key, extent, split, -0.22, 0.18)
    return jnp.clip(array, -reach, reach).astype(dtype)


def setup_inputs(seed: int = 0) -> dict:
    key_list = jax.random.split(jax.random.key(seed), 4)
    grad_out = noise(key_list[0], (REPLICAS, SEQ, D), 1.0, 6.0, ((0, 4), (1, 8)))
    hidden = noise(key_list[1], (REPLICAS, SEQ, FFS), 1.0, 6.0, ((0, 4), (1, 8)))
    down_weight = noise(key_list[2], (FFS, D), D ** -0.5, 0.09375)
    return dict(grad_out=grad_out, hidden=hidden, down_weight=down_weight)


ceiling = 448.0

def to_grid(values, peaks):
    scaled = values.astype(jnp.float32) * (ceiling / peaks)[None, :]
    magnitude = jnp.abs(scaled)
    spacing = jnp.full_like(magnitude, 2.0 ** (-9))
    for exponent in range(-5, 9):
        spacing = jnp.where(magnitude >= 2.0 ** exponent, 2.0 ** (exponent - 3), spacing)
    snapped = jnp.floor(magnitude / spacing + 0.5) * spacing
    return jnp.where(scaled < 0, -snapped, snapped).astype(jnp.bfloat16)

def reference(grad_out, hidden, down_weight):
    hidden_amax = jnp.maximum(lax.optimization_barrier(jnp.max(jnp.abs(hidden.astype(jnp.float32)), axis=1)), 1.0)
    grad_amax = jnp.maximum(lax.optimization_barrier(jnp.max(jnp.abs(grad_out.astype(jnp.float32)), axis=1)), 1.0)
    total = jnp.zeros((FFS, D), jnp.float32)
    results = []
    for replica in range(REPLICAS):
        gdata = grad_out[replica]
        hdata = hidden[replica]
        results.append(lax.dot_general(gdata, down_weight, (((1,), (1,)), ((), ())), preferred_element_type=jnp.float32).astype(jnp.bfloat16))
        hquant = to_grid(hdata, hidden_amax[replica])
        gquant = to_grid(gdata, grad_amax[replica])
        product = lax.dot_general(hquant, gquant, (((0,), (0,)), ((), ())), preferred_element_type=jnp.float32)
        total = total + product * (hidden_amax[replica] / ceiling)[:, None] * (grad_amax[replica] / ceiling)[None, :]
    weight_grad = total / jnp.sqrt(jnp.float32(SEQ * REPLICAS))
    grad_hidden = jnp.stack(results, axis=0)
    return (grad_hidden, weight_grad, hidden_amax, grad_amax)
```

```python
import jax
import jax.numpy as jnp
from jax import lax
from jax.sharding import PartitionSpec as P

ceiling = 448.0
SHARES = (3, 3, 2)


def to_grid(values, peaks):
    scaled = values.astype(jnp.float32) * (ceiling / peaks)
    level = jnp.abs(scaled) * 64.0
    power = jnp.full_like(level, 2.0 ** (-9))
    for step in (8, 4, 2, 1):
        above = level >= 2.0**step
        level = jnp.where(above, level * 2.0**-step, level)
        power = jnp.where(above, power * 2.0**step, power)
    snapped = jnp.floor(level * 8.0 + 0.5) * power
    return jnp.where(scaled < 0, -snapped, snapped).astype(jnp.bfloat16)


def local_peaks(values):
    return jnp.max(jnp.abs(values), axis=0)


def swap(value, axis, bit):
    size = lax.axis_size(axis)
    return lax.ppermute(value, axis, [(i, i ^ (1 << bit)) for i in range(size)])


def bits_of(axis):
    return lax.axis_size(axis).bit_length() - 1


def on_device(grad_out, hidden, down_weight):
    gdata = grad_out[0]
    hdata = hidden[0]
    ctx_count, dp_count = lax.axis_size("ctx"), lax.axis_size("dp")
    ctx_pos, dp_pos = lax.axis_index("ctx"), lax.axis_index("dp")
    ctx_bits, dp_bits = bits_of("ctx"), bits_of("dp")
    tokens, ff = hdata.shape
    width = gdata.shape[1]
    ff_rows, width_cols = ff // ctx_count, width // ctx_count
    outer = dp_count // 2
    unit = width // dp_count // sum(SHARES)
    edges = [unit * sum(SHARES[:c]) for c in range(len(SHARES) + 1)]
    seq_total = tokens * ctx_count * dp_count
    core = dp_pos % 2

    halves = gdata.reshape(tokens, outer, 2, width // dp_count)

    def half(values, which):
        return lax.dynamic_index_in_dim(values, which, values.ndim - 2, keepdims=False)

    gmine = half(halves, core)
    gother = swap(half(halves, 1 - core), "dp", 0)
    hother = swap(hdata, "dp", 0)

    peaks = jnp.concatenate([local_peaks(hdata), local_peaks(gdata)])
    for bit in range(ctx_bits):
        peaks = jnp.maximum(peaks, swap(peaks, "ctx", bit))
    peaks_other = swap(peaks, "dp", 0)
    peaks = jnp.maximum(peaks.astype(jnp.float32), 1.0)
    peaks_other = jnp.maximum(peaks_other.astype(jnp.float32), 1.0)
    hpeak, gpeak = peaks[:ff], peaks[ff:]

    result = lax.dot_general(
        gdata, down_weight, (((1,), (1,)), ((), ())), preferred_element_type=jnp.float32
    )
    grad_hidden = result.astype(jnp.bfloat16)[None]

    sides = []
    for h, g, pk in ((hdata, gmine, peaks), (hother, gother, peaks_other)):
        hp = pk[:ff]
        gp = half(pk[ff:].reshape(outer, 2, width // dp_count), core)
        hq = to_grid(h, hp[None, :])
        gq = to_grid(g, gp[None])
        near = [lax.dynamic_index_in_dim(gq, step ^ (dp_pos // 2), 1, keepdims=False) for step in range(outer)]
        scales = [
            lax.dynamic_index_in_dim(gp / ceiling, step ^ (dp_pos // 2), 0, keepdims=False)
            for step in range(outer)
        ]
        hq, near = lax.optimization_barrier((hq, near))
        sides.append((hq, near, hp / ceiling, scales))

    dp_list = [("dp", bit) for bit in range(1, dp_bits)]
    ctx_list = [("ctx", bit) for bit in range(ctx_bits)]
    orders = [
        dp_list + ctx_list,
        ctx_list[:2] + dp_list + ctx_list[2:],
        ctx_list[1:2] + dp_list + ctx_list[:1] + ctx_list[2:],
    ]

    def block_value(c, step):
        total = None
        cols = slice(edges[c], edges[c + 1])
        for hq, near, hs, scales in sides:
            term = lax.dot_general(
                hq, near[step][:, cols], (((0,), (0,)), ((), ())), preferred_element_type=jnp.float32
            )
            term = term * hs[:, None] * scales[step][None, cols]
            total = term if total is None else total + term
        return total.reshape(ctx_count, ff_rows, -1)

    def split(value, bit, kept):
        low = 1 << (len(kept) - 1 - kept.index(bit))
        shape = value.shape
        view = value.reshape((shape[0] // (2 * low), 2, low) + shape[1:])
        own = ctx_pos // (1 << bit) % 2
        target = (shape[0] // 2,) + shape[1:]
        keep = lax.dynamic_index_in_dim(view, own, 1, keepdims=False).reshape(target)
        send = lax.dynamic_index_in_dim(view, 1 - own, 1, keepdims=False).reshape(target)
        return keep, send

    state = []
    for c in range(len(SHARES)):
        blocks = {step: block_value(c, step) for step in reversed(range(outer))}
        state.append((blocks, list(range(ctx_bits - 1, -1, -1))))
    for stage in range(len(orders[0])):
        for c in range(len(SHARES)):
            blocks, kept = state[c]
            axis, bit = orders[c][stage]
            if axis == "dp":
                far = 1 << (bit - 1)
                blocks = {
                    step: blocks[step]
                    + swap(blocks[step ^ far].astype(jnp.bfloat16), axis, bit).astype(jnp.float32)
                    for step in blocks
                    if not step & far
                }
            else:
                pairs = {step: split(blocks[step], bit, kept) for step in blocks}
                blocks = {
                    step: keep + swap(send.astype(jnp.bfloat16), axis, bit).astype(jnp.float32)
                    for step, (keep, send) in pairs.items()
                }
                kept = [other for other in kept if other != bit]
            state[c] = (blocks, kept)
    weight_grad = jnp.concatenate(
        [blocks[0].reshape(ff_rows, -1) for blocks, _ in state], axis=1
    ) / jnp.sqrt(jnp.float32(seq_total))

    hidden_amax = lax.dynamic_slice_in_dim(hpeak, ctx_pos * ff_rows, ff_rows, 0)
    grad_amax = lax.dynamic_slice_in_dim(gpeak, ctx_pos * width_cols, width_cols, 0)
    return (grad_hidden, weight_grad, hidden_amax[None], grad_amax[None])


def solution(mesh):
    placed = (P("dp", "ctx", None), P("dp", "ctx", None), P())
    return jax.shard_map(
        on_device,
        mesh=mesh,
        in_specs=placed,
        out_specs=(P("dp", "ctx", None), P("ctx", "dp"), P("dp", "ctx"), P("dp", "ctx")),
        check_vma=False,
    )
```

```python
import jax
import jax.numpy as jnp
from jax import lax
from jax.sharding import PartitionSpec as P

ceiling = 448.0
SHARES = (3, 3, 2)


def to_grid(values, peaks):
    scaled = values.astype(jnp.float32) * (ceiling / peaks)
    level = jnp.abs(scaled) * 64.0
    power = jnp.full_like(level, 2.0 ** (-9))
    for step in (8, 4, 2, 1):
        above = level >= 2.0**step
        level = jnp.where(above, level * 2.0**-step, level)
        power = jnp.where(above, power * 2.0**step, power)
    snapped = jnp.floor(level * 8.0 + 0.5) * power
    return jnp.where(scaled < 0, -snapped, snapped).astype(jnp.bfloat16)


def local_peaks(values):
    return jnp.max(jnp.abs(values), axis=0)


def swap(value, axis, bit):
    size = lax.axis_size(axis)
    return lax.ppermute(value, axis, [(i, i ^ (1 << bit)) for i in range(size)])


def bits_of(axis):
    return lax.axis_size(axis).bit_length() - 1


def on_device(grad_out, hidden, down_weight):
    gdata = grad_out[0]
    hdata = hidden[0]
    ctx_count, dp_count = lax.axis_size("ctx"), lax.axis_size("dp")
    ctx_pos, dp_pos = lax.axis_index("ctx"), lax.axis_index("dp")
    ctx_bits, dp_bits = bits_of("ctx"), bits_of("dp")
    tokens, ff = hdata.shape
    width = gdata.shape[1]
    ff_rows, width_cols = ff // ctx_count, width // ctx_count
    outer = dp_count // 2
    unit = width // dp_count // sum(SHARES)
    edges = [unit * sum(SHARES[:c]) for c in range(len(SHARES) + 1)]
    seq_total = tokens * ctx_count * dp_count
    core = dp_pos % 2

    halves = gdata.reshape(tokens, outer, 2, width // dp_count)

    def half(values, which):
        return lax.dynamic_index_in_dim(values, which, values.ndim - 2, keepdims=False)

    gmine = half(halves, core)
    gother = swap(half(halves, 1 - core), "dp", 0)
    hother = swap(hdata, "dp", 0)

    peaks = jnp.concatenate([local_peaks(hdata), local_peaks(gdata)])
    for bit in range(ctx_bits):
        peaks = jnp.maximum(peaks, swap(peaks, "ctx", bit))
    peaks_other = swap(peaks, "dp", 0)
    peaks = jnp.maximum(peaks.astype(jnp.float32), 1.0)
    peaks_other = jnp.maximum(peaks_other.astype(jnp.float32), 1.0)
    hpeak, gpeak = peaks[:ff], peaks[ff:]

    result = lax.dot_general(
        gdata, down_weight, (((1,), (1,)), ((), ())), preferred_element_type=jnp.float32
    )
    grad_hidden = result.astype(jnp.bfloat16)[None]

    sides = []
    for h, g, pk in ((hdata, gmine, peaks), (hother, gother, peaks_other)):
        hp = pk[:ff]
        gp = half(pk[ff:].reshape(outer, 2, width // dp_count), core)
        hq = to_grid(h, hp[None, :])
        gq = to_grid(g, gp[None])
        near = [lax.dynamic_index_in_dim(gq, step ^ (dp_pos // 2), 1, keepdims=False) for step in range(outer)]
        scales = [
            lax.dynamic_index_in_dim(gp / ceiling, step ^ (dp_pos // 2), 0, keepdims=False)
            for step in range(outer)
        ]
        hq, near = lax.optimization_barrier((hq, near))
        sides.append((hq, near, hp / ceiling, scales))

    dp_list = [("dp", bit) for bit in range(1, dp_bits)]
    ctx_list = [("ctx", bit) for bit in range(ctx_bits)]
    orders = [
        dp_list + ctx_list,
        ctx_list[:2] + dp_list + ctx_list[2:],
        ctx_list[1:2] + dp_list + ctx_list[:1] + ctx_list[2:],
    ]

    def block_value(c, step):
        total = None
        cols = slice(edges[c], edges[c + 1])
        for hq, near, hs, scales in sides:
            term = lax.dot_general(
                hq, near[step][:, cols], (((0,), (0,)), ((), ())), preferred_element_type=jnp.float32
            )
            term = term * hs[:, None] * scales[step][None, cols]
            total = term if total is None else total + term
        return total.reshape(ctx_count, ff_rows, -1)

    def split(value, bit, kept):
        low = 1 << (len(kept) - 1 - kept.index(bit))
        shape = value.shape
        view = value.reshape((shape[0] // (2 * low), 2, low) + shape[1:])
        own = ctx_pos // (1 << bit) % 2
        target = (shape[0] // 2,) + shape[1:]
        keep = lax.dynamic_index_in_dim(view, own, 1, keepdims=False).reshape(target)
        send = lax.dynamic_index_in_dim(view, 1 - own, 1, keepdims=False).reshape(target)
        return keep, send

    state = []
    for c in range(len(SHARES)):
        blocks = {step: block_value(c, step) for step in reversed(range(outer))}
        state.append((blocks, list(range(ctx_bits - 1, -1, -1))))
    for stage in range(len(orders[0])):
        kept_parts, arrived = [], []
        for c in range(len(SHARES)):
            blocks, kept = state[c]
            axis, bit = orders[c][stage]
            if axis == "dp":
                far = 1 << (bit - 1)
                pairs = {step: (blocks[step], blocks[step ^ far]) for step in blocks if not step & far}
            else:
                pairs = {step: split(blocks[step], bit, kept) for step in blocks}
                kept = [other for other in kept if other != bit]
            kept_parts.append(({step: keep for step, (keep, _) in pairs.items()}, kept))
            arrived.append({step: swap(send.astype(jnp.bfloat16), axis, bit) for step, (_, send) in pairs.items()})
        arrived = lax.optimization_barrier(arrived)
        state = [
            ({step: keeps[step] + got[step].astype(jnp.float32) for step in keeps}, kept)
            for (keeps, kept), got in zip(kept_parts, arrived)
        ]
    weight_grad = jnp.concatenate(
        [blocks[0].reshape(ff_rows, -1) for blocks, _ in state], axis=1
    ) / jnp.sqrt(jnp.float32(seq_total))

    hidden_amax = lax.dynamic_slice_in_dim(hpeak, ctx_pos * ff_rows, ff_rows, 0)
    grad_amax = lax.dynamic_slice_in_dim(gpeak, ctx_pos * width_cols, width_cols, 0)
    return (grad_hidden, weight_grad, hidden_amax[None], grad_amax[None])


def solution(mesh):
    placed = (P("dp", "ctx", None), P("dp", "ctx", None), P())
    return jax.shard_map(
        on_device,
        mesh=mesh,
        in_specs=placed,
        out_specs=(P("dp", "ctx", None), P("ctx", "dp"), P("dp", "ctx"), P("dp", "ctx")),
        check_vma=False,
    )
```
